32 devices in a mesh: row: 8 (over z, y), col: 4 (over x, core).
Axes of the slice: x: 2, y: 2, z: 4, core: 2. Of those that a mesh axis runs over, the one named last changes fastest.
Arguments:
- matrix: float32 [4096, 4096], P('row', 'col'), may hold values from -0.92 to 1.92, as said below
Outputs:
- inverse: float32 [4096, 4096], P('row', 'col')
- residual_norms: float32 [4], replicated
The draws below stay inside these ranges and needn't reach their ends.
Inputs may be any that keep to these rules, and one draw needn't show every extreme that they name: matrix is exactly symmetric and positive definite; all its eigenvalues lie between 0.08 and 1.92.
All inputs are finite; a program needn't handle non-finite values.
Results may differ from the reference program's by a relative error of at most 0.0017.
The reference program's roundings to bfloat16 on the way (of `mat_low`, `cur_low` and `shift_low`) count: a program that leaves them out, or rounds other values in their place, can miss the bound.
Values may be sent and summed in bfloat16 or wider, within the bound.
A program may use at most 64 MiB of HBM per device.

```python
import jax
import jax.numpy as jnp
from jax import lax

N = 4096
ITERS = 4


def draw_matrix(key, part):
    noise_key = jax.random.fold_in(key, 17)
    noise_draw = jnp.clip(jax.random.normal(noise_key, (N, N), jnp.float32), -4.0, 4.0)
    spread = 0.9
    wigner = (noise_draw + noise_draw.T) * (0.5 / (1.4142135 * jnp.sqrt(jnp.float32(N))))
    identity = jnp.eye(N, dtype=jnp.float32)
    for polish in range(3):
        square = jnp.dot(wigner, wigner, precision=lax.Precision.HIGHEST)
        wigner = jnp.dot(wigner, 1.5 * identity - 0.5 * square, precision=lax.Precision.HIGHEST)
    shaped = 0.5 * (wigner + wigner.T)
    return identity + spread * shaped


def setup_inputs(seed: int = 0) -> dict:
    key_list = jax.random.split(jax.random.key(seed), 2)
    return {
        "matrix": draw_matrix(jax.random.fold_in(key_list[1], 71), 0),
    }


def reference(matrix):
    mat_low = matrix.astype(jnp.bfloat16)
    sq_total = jnp.sum(matrix * matrix)
    start_scale = jnp.sqrt(jnp.float32(N)) / jnp.sqrt(sq_total)
    identity = jnp.eye(N, dtype=jnp.float32)
    current = start_scale * identity
    norm_list = []
    for iteration in range(ITERS):
        cur_low = current.astype(jnp.bfloat16)
        product = jnp.dot(mat_low, cur_low, preferred_element_type=jnp.float32)
        residual = identity - product
        norm_list.append(jnp.sqrt(jnp.sum(residual * residual) / N))
        shift_low = (identity + residual).astype(jnp.bfloat16)
        current = jnp.dot(cur_low, shift_low, preferred_element_type=jnp.float32)
    return (current, jnp.stack(norm_list))
```

```python
import jax
import jax.numpy as jnp
from jax import lax
from jax.sharding import PartitionSpec as P

ITERS = 4


def rounded(value):
    return lax.reduce_precision(value, 8, 7)


def first_iterate(panel, scale_low, row_start, col_start):
    rows = row_start + lax.broadcasted_iota(jnp.int32, panel.shape, 0)
    cols = col_start + lax.broadcasted_iota(jnp.int32, panel.shape, 1)
    eye = (rows == cols).astype(jnp.float32)
    shift = rounded(eye + (eye - scale_low * panel.astype(jnp.float32)))
    return (scale_low * shift).astype(jnp.bfloat16)


def transpose_blocks(block, row_size, col_size):
    ratio = row_size // col_size
    side = block.shape[0]
    row_index = lax.axis_index("row")
    pieces = []
    for turn in range(ratio):
        pairs = []
        for row in range(row_size):
            for col in range(col_size):
                target_row = ratio * col + (row + turn) % ratio
                pairs.append((row * col_size + col, target_row * col_size + row // ratio))
        half = lax.rem(row_index + turn, ratio)
        piece = lax.dynamic_slice_in_dim(block, half * side, side, axis=1)
        pieces.append(lax.ppermute(piece, ("row", "col"), pairs).T)
    out = jnp.zeros_like(block)
    for turn in range(ratio):
        half = lax.rem(row_index - turn + ratio, ratio)
        out = lax.dynamic_update_slice_in_dim(out, pieces[turn], half * side, axis=1)
    return out


def shards(matrix):
    row_count, col_count = matrix.shape
    row_size, col_size = lax.axis_size("row"), lax.axis_size("col")
    order = col_count * col_size
    row_start = lax.axis_index("row") * row_count
    col_start = lax.axis_index("col") * col_count
    global_rows = row_start + lax.broadcasted_iota(jnp.int32, (row_count, col_count), 0)
    global_cols = col_start + lax.broadcasted_iota(jnp.int32, (row_count, col_count), 1)
    eye_block = (global_rows == global_cols).astype(jnp.float32)
    mat_low = matrix.astype(jnp.bfloat16)
    sq_total = lax.psum(jnp.sum(matrix * matrix), ("row", "col"))
    panel_rows = lax.all_gather(mat_low, "col", axis=1, tiled=True)
    panel_cols = lax.all_gather(mat_low, "row", axis=0, tiled=True)
    start_scale = jnp.sqrt(jnp.float32(order)) / jnp.sqrt(sq_total)
    scale_low = rounded(start_scale)
    residual = eye_block - scale_low * rounded(matrix)
    partial_list = [jnp.sum(residual * residual)]
    iterate_rows = first_iterate(panel_rows, scale_low, row_start, 0)
    iterate_cols = first_iterate(panel_cols, scale_low, 0, col_start)
    for iteration in range(1, ITERS):
        product = jnp.dot(iterate_rows, panel_cols, preferred_element_type=jnp.float32)
        residual = eye_block - product
        partial_list.append(jnp.sum(residual * residual))
        shift_low = (eye_block + residual).astype(jnp.bfloat16)
        current = jnp.dot(
            lax.all_gather(shift_low, "col", axis=1, tiled=True),
            iterate_cols,
            preferred_element_type=jnp.float32,
        )
        if iteration < ITERS - 1:
            cur_low = current.astype(jnp.bfloat16)
            iterate_rows = lax.all_gather(cur_low, "col", axis=1, tiled=True)
            iterate_cols = lax.all_gather(cur_low, "row", axis=0, tiled=True)
    summed = lax.psum(jnp.stack(partial_list), ("row", "col"))
    residual_norms = jnp.sqrt(summed / order)
    return (transpose_blocks(current, row_size, col_size), residual_norms)


def solution(mesh):
    in_specs = (P("row", "col"),)
    out_specs = (P("row", "col"), P())
    return jax.shard_map(shards, mesh=mesh, in_specs=in_specs, out_specs=out_specs, check_vma=False)
```

```python
import jax
import jax.numpy as jnp
from jax import lax
from jax.sharding import PartitionSpec as P

ITERS = 4


def rounded(value):
    return lax.reduce_precision(value, 8, 7)


def first_iterate(panel, scale_low, row_start, col_start):
    rows = row_start + lax.broadcasted_iota(jnp.int32, panel.shape, 0)
    cols = col_start + lax.broadcasted_iota(jnp.int32, panel.shape, 1)
    eye = (rows == cols).astype(jnp.float32)
    shift = rounded(eye + (eye - scale_low * panel.astype(jnp.float32)))
    return (scale_low * shift).astype(jnp.bfloat16)


def transpose_blocks(block, row_size, col_size):
    ratio = row_size // col_size
    side = block.shape[0]
    row_index = lax.axis_index("row")
    pieces = []
    for turn in range(ratio):
        pairs = []
        for row in range(row_size):
            for col in range(col_size):
                target_row = ratio * col + (row + turn) % ratio
                pairs.append((row * col_size + col, target_row * col_size + row // ratio))
        half = lax.rem(row_index + turn, ratio)
        piece = lax.dynamic_slice_in_dim(block, half * side, side, axis=1)
        pieces.append(lax.ppermute(piece, ("row", "col"), pairs).T)
    out = jnp.zeros_like(block)
    for turn in range(ratio):
        half = lax.rem(row_index - turn + ratio, ratio)
        out = lax.dynamic_update_slice_in_dim(out, pieces[turn], half * side, axis=1)
    return out


def gather_cols(block, col_size):
    width = block.shape[1]
    col_index = lax.axis_index("col")
    panel = jnp.zeros((block.shape[0], width * col_size), block.dtype)
    panel = lax.dynamic_update_slice_in_dim(panel, block, col_index * width, axis=1)
    moved = []
    for turn in range(1, col_size):
        pairs = [(col, (col + turn) % col_size) for col in range(col_size)]
        moved.append(lax.ppermute(block, "col", pairs))
    for turn in range(1, col_size):
        owner = lax.rem(col_index - turn + col_size, col_size)
        panel = lax.dynamic_update_slice_in_dim(panel, moved[turn - 1], owner * width, axis=1)
    return panel


def shards(matrix):
    row_count, col_count = matrix.shape
    row_size, col_size = lax.axis_size("row"), lax.axis_size("col")
    order = col_count * col_size
    row_start = lax.axis_index("row") * row_count
    col_start = lax.axis_index("col") * col_count
    global_rows = row_start + lax.broadcasted_iota(jnp.int32, (row_count, col_count), 0)
    global_cols = col_start + lax.broadcasted_iota(jnp.int32, (row_count, col_count), 1)
    eye_block = (global_rows == global_cols).astype(jnp.float32)
    mat_low = matrix.astype(jnp.bfloat16)
    sq_total = lax.psum(jnp.sum(matrix * matrix), ("row", "col"))
    panel_rows = gather_cols(mat_low, col_size)
    panel_cols = lax.all_gather(mat_low, "row", axis=0, tiled=True)
    start_scale = jnp.sqrt(jnp.float32(order)) / jnp.sqrt(sq_total)
    scale_low = rounded(start_scale)
    residual = eye_block - scale_low * rounded(matrix)
    partial_list = [jnp.sum(residual * residual)]
    iterate_rows = first_iterate(panel_rows, scale_low, row_start, 0)
    iterate_cols = first_iterate(panel_cols, scale_low, 0, col_start)
    for iteration in range(1, ITERS):
        product = jnp.dot(iterate_rows, panel_cols, preferred_element_type=jnp.float32)
        residual = eye_block - product
        partial_list.append(jnp.sum(residual * residual))
        shift_low = (eye_block + residual).astype(jnp.bfloat16)
        current = jnp.dot(
            gather_cols(shift_low, col_size),
            iterate_cols,
            preferred_element_type=jnp.float32,
        )
        if iteration < ITERS - 1:
            cur_low = current.astype(jnp.bfloat16)
            iterate_cols = lax.all_gather(cur_low, "row", axis=0, tiled=True)
            iterate_rows = gather_cols(cur_low, col_size)
    summed = lax.psum(jnp.stack(partial_list), ("row", "col"))
    residual_norms = jnp.sqrt(summed / order)
    return (transpose_blocks(current, row_size, col_size), residual_norms)


def solution(mesh):
    in_specs = (P("row", "col"),)
    out_specs = (P("row", "col"), P())
    return jax.shard_map(shards, mesh=mesh, in_specs=in_specs, out_specs=out_specs, check_vma=False)
```
